32 devices in a mesh: level: 4 (over x, core), body: 8 (over z, y).
Axes of the slice: x: 2, y: 2, z: 4, core: 2. Of those that a mesh axis runs over, the one named last changes fastest.
Arguments:
- state: float32 [4, 6, 8192], P('level', None, 'body'), may hold values from -14 to 14
- history: float32 [4, 3, 6, 8192], P('level', None, None, 'body'), may hold values from -6 to 6
- masses: float32 [8192], P('body'), may hold values from 0.25 to 4
Outputs:
- final_state: float32 [4, 6, 8192], P('level', None, 'body')
The draws below stay inside these ranges and needn't reach their ends.
All inputs are finite; a program needn't handle non-finite values.
Results may differ from the reference program's by a relative error of at most 0.0001.
Values sent between devices are 32-bit elements; how exact they have to be, the bound alone decides.
No kernel may reach another device: no remote copies, remote signals or barrier semaphores. Data moves between devices by JAX's collectives and lax.ppermute only.
A program may use at most 64 MiB of HBM per device.

```python
import math
import jax
import jax.numpy as jnp
from jax import lax

LEVELS = 4
STEPS = 4
BODIES = 8192


def draw_state(key, part):
    key = jax.random.fold_in(key, 17)
    keys = jax.random.split(key, 6)
    positions = jnp.clip(jax.random.normal(keys[4], (LEVELS, 3, BODIES), jnp.float32), -6.0, 6.0)
    velocities = jnp.clip(jax.random.normal(keys[5], (LEVELS, 3, BODIES), jnp.float32), -6.0, 6.0)
    return jnp.concatenate([positions, velocities], axis=1).astype(jnp.float32)


def levels(key, shape, pieces, low, high):
    gain = 1.0
    for axis_at, parts in pieces:
        draws = jax.random.uniform(jax.random.fold_in(jax.random.fold_in(key, 6), axis_at), (parts,), jnp.float32, low / len(pieces), high / len(pieces))
        gain = gain * jnp.repeat(jnp.exp(draws), shape[axis_at] // parts).reshape((-1,) + (1,) * (len(shape) - 1 - axis_at))
    return gain


def gaussian(rng, extent, scale, bound, cuts=(), held_as=jnp.bfloat16):
    entries = jax.random.normal(rng, extent, jnp.float32) * scale
    if len(cuts) > 0:
        entries = levels(rng, extent, cuts, -0.22, 0.18) * entries
    return jnp.clip(entries, min=-bound, max=bound).astype(held_as)


def setup_inputs(seed: int = 0) -> dict:
    arg_keys = jax.random.split(jax.random.key(seed), 4)
    return {
        "state": draw_state(jax.random.fold_in(arg_keys[3], 71), 0),
        "history": gaussian(arg_keys[1], (LEVELS, 3, 6, BODIES), 1.0, 6.0, ((0, 4), (3, 8)), jnp.float32),
        "masses": jnp.clip(jnp.exp(math.log(4.0) - 2.7725887 * jax.random.uniform(arg_keys[2], (BODIES,), jnp.float32) ** levels(arg_keys[2], (BODIES,), ((0, 8),), -0.2, 0.2)), 0.25, 4.0),
    }


SOFTEN = 0.05
DELTA = 0.05
COUPLING = 512.0

def accelerate(positions, masses):
    block_size = min(BODIES, 1024)

    def one_block(targets):
        offsets = positions[:, None, :] - targets[:, :, None]
        distance = lax.optimization_barrier(jnp.sum(offsets * offsets, axis=0)) + SOFTEN
        weight = masses[None, :] / (distance * jnp.sqrt(distance))
        return lax.optimization_barrier(jnp.sum(offsets * weight[None], axis=2))
    tile_list = positions.reshape(3, BODIES // block_size, block_size).transpose(1, 0, 2)
    pull_tiles = lax.map(one_block, tile_list)
    return pull_tiles.transpose(1, 0, 2).reshape(3, BODIES) * (COUPLING / BODIES)

def reference(state, history, masses):
    current = state
    stored = history
    for repeat_index in range(STEPS):
        forces = jnp.stack([jnp.concatenate([current[level_index, 3:6], accelerate(current[level_index, 0:3], masses)], axis=0) for level_index in range(LEVELS)])
        updated = [current[0] + DELTA * forces[0]]
        retained = [stored[0]]
        for level_index in range(1, LEVELS):
            history_rows = stored[level_index]
            quadrature = history_rows[0] / 24.0 - 5.0 * history_rows[1] / 24.0 + 19.0 * history_rows[2] / 24.0 + 9.0 * forces[level_index - 1] / 24.0
            updated.append(current[level_index] + DELTA * (forces[level_index] - history_rows[2]) + DELTA * quadrature)
            retained.append(jnp.stack([history_rows[1], history_rows[2], forces[level_index - 1]]))
        current = jnp.stack(updated)
        stored = jnp.stack(retained)
    return current
```

```python
import jax
import jax.numpy as jnp
from jax import lax
from jax.experimental import pallas as pl
from jax.experimental.pallas import tpu as pltpu
from jax.sharding import PartitionSpec as P

SOFTEN = 0.05
DELTA = 0.05
COUPLING = 512.0

F32, BF16 = jnp.float32, jnp.bfloat16
TILE = 256
PIECE = 32
LANES = 128
HALF = TILE // PIECE // 2


def split3(x):
    first = x.astype(BF16).astype(F32)
    rest = x - first
    second = rest.astype(BF16).astype(F32)
    return first, second, rest - second


def pull_kernel(own_count, blocks, row, own_ref, src_ref, mu_ref, out_ref, s_ref, p_ref, t_ref, w_ref):
    passes = own_count // (2 * TILE)
    chunks = blocks * own_count // TILE
    pieces = TILE // PIECE
    units = range(2)

    def main(*accs):
        accs = list(accs)
        d_acc = [[[accs.pop(0) for _ in range(pieces)] for _ in range(2)] for _ in units]
        o_acc = [[[accs.pop(0) for _ in range(2)] for _ in range(passes)] for _ in units]

        own = own_ref[...]
        square = jnp.sum(own * own, axis=0, keepdims=True)
        zero8 = jnp.zeros((8, own_count), F32)
        target = jnp.concatenate([own, jnp.ones((1, own_count), F32), square, zero8[0:3]], axis=0)
        stack = list(split3(target)) * 3
        stack = stack + [zero8] * (TILE // 8 - len(stack))
        t_ref[...] = jnp.concatenate(stack, axis=0).astype(BF16)

        def prepare(block, carry):
            pos = src_ref[block, row:row + 3, :]
            mu = mu_ref[block, 6:7, :]
            norm = jnp.sum(pos * pos, axis=0, keepdims=True)
            source = jnp.concatenate([-2.0 * mu * pos, mu * (norm + SOFTEN), mu, zero8[0:3]], axis=0)
            s1, s2, s3 = split3(source)
            p1, p2, p3 = split3(jnp.concatenate([pos, jnp.ones((1, own_count), F32), zero8[0:4]], axis=0))
            stacked = jnp.concatenate([s1] * 3 + [s2] * 3 + [s3] * 3 + [zero8] * 7, axis=0)
            start = pl.multiple_of(block * own_count, own_count)
            for lane in range(0, own_count, LANES):
                s_ref[pl.ds(start + lane, LANES), :] = stacked[:, lane:lane + LANES].T.astype(BF16)
            p_ref[0:16, pl.ds(start, own_count)] = jnp.concatenate([p1, p2], axis=0).astype(BF16)
            p_ref[16:32, pl.ds(start, own_count)] = jnp.concatenate([p3, zero8], axis=0).astype(BF16)
            return carry

        lax.fori_loop(0, blocks, prepare, 0)

        def push_targets(unit, which):
            low = (unit * passes + which) * TILE
            pltpu.matmul_push_rhs(t_ref[:, low:low + TILE], staging_register=0, mxu_index=unit)

        def distances(unit, slot, piece, chunk, latch):
            start = chunk * TILE + piece * PIECE
            if not isinstance(chunk, int):
                start = pl.multiple_of(start, PIECE)
            rows = jnp.concatenate([s_ref[pl.ds(start, PIECE), :], jnp.zeros((PIECE, LANES), BF16)], axis=1)
            pltpu.matmul_acc_lhs(d_acc[unit][slot][piece], rows, load_staged_rhs=0 if latch else None)

        def weigh(unit, slot, piece):
            inverse = lax.rsqrt(pltpu.matmul_pop(d_acc[unit][slot][piece]))
            weight = inverse * inverse * inverse
            high = weight.astype(BF16)
            low = (weight - high.astype(F32)).astype(BF16)
            w_ref[slot, unit, 0, piece * PIECE:(piece + 1) * PIECE, :] = high
            w_ref[slot, unit, 1, piece * PIECE:(piece + 1) * PIECE, :] = low

        def push_weights(unit, slot, part):
            pltpu.matmul_push_rhs(w_ref[slot, unit, part], staging_register=1, mxu_index=unit)

        def pull(unit, part, which, chunk):
            start = chunk * TILE
            if not isinstance(chunk, int):
                start = pl.multiple_of(start, TILE)
            rows = p_ref[0:16 if part else 32, pl.ds(start, TILE)]
            pltpu.matmul_acc_lhs(o_acc[unit][which][part], rows, load_staged_rhs=1)

        def step(slot, last, following, which):
            for part in range(2):
                if following is not None:
                    for unit in units:
                        push_targets(unit, which)
                if last is not None:
                    for unit in units:
                        push_weights(unit, 1 - slot, part)
                for piece in range(part * HALF, (part + 1) * HALF):
                    for unit in units:
                        weigh(unit, slot, piece)
                        if following is not None:
                            distances(unit, slot, piece, following, piece == part * HALF)
                if last is not None:
                    for unit in units:
                        pull(unit, part, *last)

        for unit in units:
            for acc in sum(d_acc[unit], []) + sum(o_acc[unit], []):
                pltpu.matmul_pop(acc)
            push_targets(unit, 0)
        for slot in range(2):
            for unit in units:
                for piece in range(pieces):
                    distances(unit, slot, piece, slot, slot == 0 and piece == 0)
        for which in range(passes):
            step(0, (which - 1, chunks - 1) if which else None, 2, which)
            step(1, (which, 0), 3, which)

            def pair(index, carry):
                step(0, (which, 2 * index - 1), 2 * index + 2, which)
                step(1, (which, 2 * index), 2 * index + 3, which)
                return carry

            lax.fori_loop(1, chunks // 2 - 1, pair, 0)
            more = which + 1 < passes
            step(0, (which, chunks - 3), 0 if more else None, which + 1)
            step(1, (which, chunks - 2), 1 if more else None, which + 1)
        for part in range(2):
            for unit in units:
                push_weights(unit, 1, part)
                pull(unit, part, passes - 1, chunks - 1)
        for unit in units:
            for which in range(passes):
                a = pltpu.matmul_pop(o_acc[unit][which][0])
                b = pltpu.matmul_pop(o_acc[unit][which][1])
                total = (a[0:8] + b[0:8]) + (a[8:16] + b[8:16]) + a[16:24]
                low = (unit * passes + which) * TILE
                pulled = total[0:3] - own_ref[:, low:low + TILE] * total[3:4]
                out_ref[:, low:low + TILE] = pulled * (COUPLING / (blocks * own_count))

    shapes = []
    for unit in units:
        shapes += [pltpu.ACC(unit)((PIECE, TILE), F32)] * (2 * pieces)
    for unit in units:
        shapes += [pltpu.ACC(unit)((32, TILE), F32), pltpu.ACC(unit)((16, TILE), F32)] * passes
    pl.run_scoped(main, *shapes)


def acceleration(own, sources, scales, row):
    own_count = own.shape[1]
    blocks = sources.shape[0]
    count = blocks * own_count
    whole = pl.BlockSpec(memory_space=pltpu.VMEM)

    def kernel(*refs):
        pull_kernel(own_count, blocks, row, *refs)

    return pl.pallas_call(
        kernel,
        out_shape=jax.ShapeDtypeStruct((3, own_count), F32),
        in_specs=[whole] * 3,
        out_specs=whole,
        scratch_shapes=[
            pltpu.VMEM((count, LANES), BF16),
            pltpu.VMEM((32, count), BF16),
            pltpu.VMEM((TILE, own_count), BF16),
            pltpu.VMEM((2, 2, 2, TILE, TILE), BF16),
        ],
        cost_estimate=pl.CostEstimate(
            flops=20 * own_count * count, bytes_accessed=32 * count, transcendentals=own_count * count
        ),
    )(own, sources, scales)


def everyone(rows, axis):
    copies = jnp.broadcast_to(rows[None], (lax.axis_size(axis),) + rows.shape)
    return lax.all_to_all(copies, axis, 0, 0)


def on_device(state, history, masses):
    level = lax.axis_index("level")
    above = level > 0
    p0, v0 = state[0, 0:3], state[0, 3:6]
    stored = jnp.where(above, history[0], 0.0)
    hp = [stored[k, 0:3] for k in range(3)]
    hv = [stored[k, 3:6] for k in range(3)]

    def lower(rows, gathered, distance):
        picked = lax.dynamic_index_in_dim(gathered, jnp.maximum(level - distance, 0), 0, False)
        return jnp.where(level >= distance, picked, 0.0)

    def advance(value, force, past, newest):
        old, older, oldest = past[2], past[1], past[0]
        return value + DELTA * (force - old) + DELTA * (
            oldest / 24.0 - 5.0 * older / 24.0 + 19.0 * old / 24.0 + 9.0 * newest / 24.0
        )

    w0 = lower(None, lax.all_gather(v0, "level"), 1)
    p1 = advance(p0, v0, hp, w0)
    scale = jnp.exp2(jnp.log2(masses) * (-2.0 / 3.0))[None]
    first = everyone(jnp.concatenate([p0, p1, scale, scale], axis=0), "body")
    a0 = acceleration(p0, first, first, 0)
    a1 = acceleration(p1, first, first, 3)

    zero = jnp.zeros_like(v0)
    x1 = advance(v0, a0, hv, zero)
    x2 = advance(x1, a1, [hv[1], hv[2], zero], zero)
    gathered = lax.all_gather(jnp.concatenate([a0, a1, x1, x2], axis=0), "level")
    below = lower(None, gathered, 1)
    second = lower(None, gathered, 2)
    b0, b1 = below[0:3], below[3:6]
    w1 = below[6:9] + DELTA * (9.0 / 24.0) * second[0:3]
    w2 = below[9:12] + DELTA * ((4.0 / 24.0) * second[0:3] + (9.0 / 24.0) * second[3:6])
    v1 = advance(v0, a0, hv, b0)
    v2 = advance(v1, a1, [hv[1], hv[2], b0], b1)
    p2 = advance(p1, v1, [hp[1], hp[2], w0], w1)
    p3 = advance(p2, v2, [hp[2], w0, w1], w2)
    later = everyone(jnp.concatenate([p2, p3, p3[0:2]], axis=0), "body")
    a2 = acceleration(p2, later, first, 0)
    a3 = acceleration(p3, later, first, 3)

    x3 = advance(v2, a2, [hv[2], b0, b1], zero)
    gathered = lax.all_gather(jnp.concatenate([a2, a3, x3], axis=0), "level")
    below = lower(None, gathered, 1)
    second = lower(None, gathered, 2)
    b2, b3 = below[0:3], below[3:6]
    w3 = below[6:9] + DELTA * (9.0 / 24.0) * second[0:3]
    v3 = advance(v2, a2, [hv[2], b0, b1], b2)
    v4 = advance(v3, a3, [b0, b1, b2], b3)
    p4 = advance(p3, v3, [w0, w1, w2], w3)
    return jnp.concatenate([p4, v4], axis=0)[None]


def solution(mesh):
    placed = (P("level", None, "body"), P("level", None, None, "body"), P("body"))
    return jax.shard_map(
        on_device, mesh=mesh, in_specs=placed, out_specs=P("level", None, "body"), check_vma=False
    )
```

```python
import jax
import jax.numpy as jnp
from jax import lax
from jax.experimental import pallas as pl
from jax.experimental.pallas import tpu as pltpu
from jax.sharding import PartitionSpec as P

SOFTEN = 0.05
DELTA = 0.05
COUPLING = 512.0
STEP = DELTA * 9.0 / 24.0

F32, BF16 = jnp.float32, jnp.bfloat16
TILE = 256
PIECE = 16
UNROLL = 4
LANES = 128


def split3(x):
    first = x.astype(BF16).astype(F32)
    rest = x - first
    second = rest.astype(BF16).astype(F32)
    return first, second, rest - second


def pull_kernel(own_count, blocks, row, own_ref, src_ref, mu_ref, out_ref, s_ref, p_ref, t_ref, w_ref):
    tiles = own_count // TILE
    chunks = blocks * own_count // TILE
    pieces = TILE // PIECE

    def main(*accs):
        accs = list(accs)
        d_acc = [[accs.pop(0) for _ in range(pieces)] for _ in range(2)]
        o_acc = [[accs.pop(0) for _ in range(2)] for _ in range(tiles)]

        own = own_ref[...]
        square = jnp.sum(own * own, axis=0, keepdims=True)
        zero8 = jnp.zeros((8, own_count), F32)
        one = jnp.ones((1, own_count), F32)
        t1, t2, t3 = split3(jnp.concatenate([own, one, square, zero8[0:3]], axis=0))
        t_ref[...] = jnp.concatenate([t1, t2, t3, t1, t2, t1] + [zero8] * (TILE // 8 - 6), axis=0)

        def prepare(block, carry):
            pos = src_ref[block, row:row + 3, :]
            mu = mu_ref[block, 6:7, :]
            norm = jnp.sum(pos * pos, axis=0, keepdims=True)
            s1, s2, s3 = split3(jnp.concatenate([-2.0 * mu * pos, mu * (norm + SOFTEN), mu, zero8[0:3]], axis=0))
            stacked = jnp.concatenate([s1, s1, s1, s2, s2, s3] + [zero8] * 10, axis=0)
            start = pl.multiple_of(block * own_count, own_count)
            for lane in range(0, own_count, LANES):
                s_ref[pl.ds(start + lane, LANES), :] = stacked[:, lane:lane + LANES].T
            p1, p2, p3 = split3(jnp.concatenate([pos, one, zero8[0:4]], axis=0))
            p_ref[:, pl.ds(start, own_count)] = jnp.concatenate([p1, p2, p3], axis=0)
            return carry

        lax.fori_loop(0, blocks, prepare, 0)

        def push_targets(tile):
            pltpu.matmul_push_rhs(t_ref[:, tile * TILE:(tile + 1) * TILE], staging_register=0, mxu_index=0)

        def distances(slot, piece, chunk, latch):
            start = chunk * TILE + piece * PIECE
            if not isinstance(chunk, int):
                start = pl.multiple_of(start, PIECE)
            rows = jnp.concatenate([s_ref[pl.ds(start, PIECE), :], jnp.zeros((PIECE, LANES), F32)], axis=1)
            pltpu.matmul_acc_lhs(d_acc[slot][piece], rows, load_staged_rhs=0 if latch else None)

        def weigh(slot, piece):
            inverse = lax.rsqrt(pltpu.matmul_pop(d_acc[slot][piece]))
            weight = inverse * inverse * inverse
            high = weight.astype(BF16).astype(F32)
            w_ref[slot, 0, piece * PIECE:(piece + 1) * PIECE, :] = high
            w_ref[slot, 1, piece * PIECE:(piece + 1) * PIECE, :] = weight - high

        def pull(slot, part, tile, chunk):
            start = chunk * TILE
            if not isinstance(chunk, int):
                start = pl.multiple_of(start, TILE)
            pltpu.matmul_push_rhs(w_ref[slot, part], staging_register=part, mxu_index=1)
            rows = p_ref[0:16 if part else 24, pl.ds(start, TILE)]
            pltpu.matmul_acc_lhs(o_acc[tile][part], rows, load_staged_rhs=part)

        def step(slot, last, following, new_tile=None):
            if new_tile is not None:
                push_targets(new_tile)
            for piece in range(pieces):
                if last is not None and piece % (pieces // 2) == 0:
                    pull(1 - slot, piece // (pieces // 2), *last)
                weigh(slot, piece)
                if following is not None:
                    distances(slot, piece, following, new_tile is not None and piece == 0)

        for acc in d_acc[0] + d_acc[1] + sum(o_acc, []):
            pltpu.matmul_pop(acc)
        push_targets(0)
        for slot in range(2):
            for piece in range(pieces):
                distances(slot, piece, slot, slot + piece == 0)
        for tile in range(tiles):
            step(0, (tile - 1, chunks - 1) if tile else None, 2)
            step(1, (tile, 0), 3)
            spare = (chunks - 4) % UNROLL

            def middle(first, steps):
                for index in range(steps):
                    step(index % 2, (tile, first + index - 1), first + index + 2)

            def group(index, carry):
                middle(2 + spare + index * UNROLL, UNROLL)
                return carry

            middle(2, spare)
            lax.fori_loop(0, (chunks - 4) // UNROLL, group, 0)
            more = tile + 1 < tiles
            step(0, (tile, chunks - 3), 0 if more else None, tile + 1 if more else None)
            step(1, (tile, chunks - 2), 1 if more else None)
        for part in range(2):
            pull(1, part, tiles - 1, chunks - 1)
        for tile in range(tiles):
            a = pltpu.matmul_pop(o_acc[tile][0])
            b = pltpu.matmul_pop(o_acc[tile][1])
            total = (a[0:8] + b[0:8]) + (a[8:16] + b[8:16]) + a[16:24]
            low = tile * TILE
            pulled = total[0:3] - own_ref[:, low:low + TILE] * total[3:4]
            out_ref[:, low:low + TILE] = pulled * (COUPLING / (blocks * own_count))

    shapes = [pltpu.ACC(0)((PIECE, TILE), F32)] * (2 * pieces)
    shapes += [pltpu.ACC(1)((24, TILE), F32), pltpu.ACC(1)((16, TILE), F32)] * tiles
    pl.run_scoped(main, *shapes)


def acceleration(own, sources, scales, row):
    own_count = own.shape[1]
    blocks = sources.shape[0]
    count = blocks * own_count
    whole = pl.BlockSpec(memory_space=pltpu.VMEM)

    def kernel(*refs):
        pull_kernel(own_count, blocks, row, *refs)

    return pl.pallas_call(
        kernel,
        out_shape=pltpu.VMEM((3, own_count), F32),
        in_specs=[whole] * 3,
        out_specs=whole,
        scratch_shapes=[
            pltpu.VMEM((count, LANES), F32),
            pltpu.VMEM((24, count), F32),
            pltpu.VMEM((TILE, own_count), F32),
            pltpu.VMEM((2, 2, TILE, TILE), F32),
        ],
        cost_estimate=pl.CostEstimate(
            flops=6 * TILE * own_count * count, bytes_accessed=32 * count, transcendentals=own_count * count
        ),
    )(*(pltpu.with_memory_space_constraint(x, pltpu.VMEM) for x in (own, sources, scales)))


def everyone(rows, axis):
    copies = jnp.broadcast_to(rows[None], (lax.axis_size(axis),) + rows.shape)
    return lax.all_to_all(copies, axis, 0, 0)


def on_device(state, history, masses):
    level = lax.axis_index("level")
    above = level > 0
    p0, v0 = state[0, 0:3], state[0, 3:6]
    stored = jnp.where(above, history[0], 0.0)
    hp = [stored[k, 0:3] for k in range(3)]
    hv = [stored[k, 3:6] for k in range(3)]

    def lower(gathered, distance):
        picked = lax.dynamic_index_in_dim(gathered, jnp.maximum(level - distance, 0), 0, False)
        return jnp.where(level >= distance, picked, 0.0)

    def advance(value, force, past, newest):
        old, older, oldest = past[2], past[1], past[0]
        return value + DELTA * (force - old) + DELTA * (
            oldest / 24.0 - 5.0 * older / 24.0 + 19.0 * old / 24.0 + 9.0 * newest / 24.0
        )

    w0 = lower(lax.all_gather(v0, "level"), 1)
    p1 = advance(p0, v0, hp, w0)
    scale = jnp.exp2(jnp.log2(masses) * (-2.0 / 3.0))[None]
    first = everyone(jnp.concatenate([p0, p1, scale, scale], axis=0), "body")
    a0 = acceleration(p0, first, first, 0)
    a1 = acceleration(p1, first, first, 3)

    zero = jnp.zeros_like(v0)
    x1 = advance(v0, a0, hv, zero)
    x2 = advance(x1, a1, [hv[1], hv[2], zero], zero)
    gathered = lax.all_gather(jnp.concatenate([a0, a1, x1, x2], axis=0), "level")
    below = lower(gathered, 1)
    second = lower(gathered, 2)
    b0, b1 = below[0:3], below[3:6]
    w1 = below[6:9] + DELTA * (9.0 / 24.0) * second[0:3]
    w2 = below[9:12] + DELTA * ((4.0 / 24.0) * second[0:3] + (9.0 / 24.0) * second[3:6])
    v1 = advance(v0, a0, hv, b0)
    v2 = advance(v1, a1, [hv[1], hv[2], b0], b1)
    p2 = advance(p1, v1, [hp[1], hp[2], w0], w1)
    p3 = advance(p2, v2, [hp[2], w0, w1], w2)
    later = everyone(jnp.concatenate([p2, p3, p3[0:2]], axis=0), "body")
    a2 = acceleration(p2, later, first, 0)
    a3 = acceleration(p3, later, first, 3)

    x3 = advance(v2, a2, [hv[2], b0, b1], zero)
    gathered = lax.all_gather(jnp.concatenate([a2, a3, x3], axis=0), "level")
    below = lower(gathered, 1)
    second = lower(gathered, 2)
    b2, b3 = below[0:3], below[3:6]
    w3 = below[6:9] + DELTA * (9.0 / 24.0) * second[0:3]
    v3 = advance(v2, a2, [hv[2], b0, b1], b2)
    v4 = advance(v3, a3, [b0, b1, b2], b3)
    p4 = advance(p3, v3, [w0, w1, w2], w3)
    return jnp.concatenate([p4, v4], axis=0)[None]


def solution(mesh):
    placed = (P("level", None, "body"), P("level", None, None, "body"), P("body"))
    return jax.shard_map(
        on_device, mesh=mesh, in_specs=placed, out_specs=P("level", None, "body"), check_vma=False
    )
```
